256 devices in a mesh: ctx: 32 (over y, z), head: 8 (over x, core).
Axes of the slice: x: 4, y: 4, z: 8, core: 2. Of those that a mesh axis runs over, the one named last changes fastest.
Arguments:
- q_first: bfloat16 [768, 4096], P('head'), may hold values from -24 to 24
- q_second: bfloat16 [768, 4096], P('head'), may hold values from -24 to 24
- k_cache: bfloat16 [131072, 16, 128], P('ctx', 'head'), may hold values from -8 to 8
- v_cache: bfloat16 [131072, 16, 128], P('ctx', 'head'), may hold values from -6 to 6
- kept_blocks: int32 [32, 32], P('ctx'), may hold values from 0 to 31, as said below
- kept_count: int32 [32], P('ctx'), may hold values from 1 to 32, 256 in all
Outputs:
- out_first: bfloat16 [768, 4096], P('ctx', 'head')
- out_second: bfloat16 [768, 4096], P('ctx', 'head')
The draws below stay inside these ranges and needn't reach their ends.
Inputs may be any that keep to these rules, and one draw needn't show every extreme that they name: `kept_blocks`: row s lists distinct block numbers of shard s; only its first kept_count[s] entries are kept. `kept_count`: the counts sum to 256; the largest is 32.
All inputs are finite; a program needn't handle non-finite values. No bound on the sum of `kept_count` on one device may be relied on, other than what follows from the above.
Results may differ from the reference program's by a relative error of at most 0.022.
Values may be sent and summed in bfloat16 or wider, within the bound.
A program may use at most 64 MiB of HBM per device.

```python
import math
import jax
import jax.numpy as jnp
import numpy as np
from jax import lax

QH = 32
KVH = 16
HD = 128
QPS = 168
ROWS = 768
BLK = 128
BLK_DEV = 32
SHARDS = 32
CTX_DEV = 4096
CTX = 131072
KEEP_MAX = 32
KEPT = 256


def kept_table(key):
    shard_total = CTX // CTX_DEV
    split_keys = jax.random.split(key, shard_total)
    table = jax.vmap(lambda split_key: jax.random.permutation(split_key, BLK_DEV)[:KEEP_MAX])(split_keys)
    return table.astype(jnp.int32)


def draw_kept_blocks(key, part):
    return kept_table(jax.random.fold_in(key, 11))


def draw_k_cache(key, part):
    drawn = jax.random.normal(jax.random.fold_in(key, 3), (CTX, KVH, HD), jnp.float32)
    return jnp.clip(drawn, -8.0, 8.0).astype(jnp.bfloat16)


def query_draw(key, which):
    spread = 3.0 * math.sqrt(QPS / HD)
    drawn = jax.random.normal(jax.random.fold_in(key, 20 + which), (ROWS, QH * HD), jnp.float32) * spread
    return jnp.clip(drawn, -24.0, 24.0).astype(jnp.bfloat16)


def draw_q_first(key, part):
    return query_draw(key, 0)


def draw_q_second(key, part):
    return query_draw(key, 1)


def level_of(key, extent, cuts, smallest, largest):
    factor_of = 1.0
    for axis_at, blocks in cuts:
        heights = jax.random.uniform(jax.random.fold_in(jax.random.fold_in(key, 6), axis_at), (blocks,), jnp.float32, smallest / len(cuts), largest / len(cuts))
        factor_of = factor_of * jnp.repeat(jnp.exp(heights), extent[axis_at] // blocks).reshape((-1,) + (1,) * (len(extent) - 1 - axis_at))
    return factor_of


def profile(number_of, total, most, skew):
    loads = [(1 << 20) // math.isqrt(grade ** skew) + 1 for grade in range(2, number_of + 1)]
    surplus, holding = total - most - (number_of - 1), [1] * (number_of - 1)
    while surplus > 0:
        free = [i for i in range(number_of - 1) if holding[i] < most]
        whole, left = sum([loads[i] for i in free]), surplus
        for i in free:
            addition = min(most - holding[i], max(1, left * loads[i] // whole), surplus)
            holding[i] = holding[i] + addition
            surplus = surplus - addition
    return np.array([most] + holding)


def ragged(own_key, amount, total, reach, skew):
    if amount == 2:
        one = jax.random.randint(own_key, (), max(1, total - reach), min(reach, total - 1) + 1)
        return jnp.stack([one, total - one])
    lengths = jnp.asarray(profile(amount, total, reach, skew), jnp.int32)
    pairs = (amount - 1) // 2
    giver, sink = lengths[1:1 + 2 * pairs:2], lengths[2:2 + 2 * pairs:2]
    room = jnp.minimum(giver - 1, reach - sink)
    moved = jax.random.randint(jax.random.fold_in(own_key, 1), (pairs,), 0, 1 << 20) % (room + 1)
    lengths = lengths.at[1:1 + 2 * pairs:2].set(giver - moved).at[2:2 + 2 * pairs:2].set(sink + moved)
    return lengths[jax.random.permutation(jax.random.fold_in(own_key, 2), amount)]


def bell_draw(key, dims, deviation, most, cuts=(), held_as=jnp.bfloat16):
    entries = jax.random.normal(key, dims, jnp.float32) * deviation
    if len(cuts) > 0:
        entries = level_of(key, dims, cuts, -0.22, 0.18) * entries
    return jnp.clip(entries, min=-most, max=most).astype(held_as)


def setup_inputs(seed: int = 0) -> dict:
    splits = jax.random.split(jax.random.key(seed), 7)
    return {
        "q_first": draw_q_first(jax.random.fold_in(splits[6], 71), 0),
        "q_second": draw_q_second(jax.random.fold_in(splits[6], 71), 0),
        "k_cache": draw_k_cache(jax.random.fold_in(splits[6], 71), 0),
        "v_cache": bell_draw(splits[3], (CTX, KVH, HD), 1.0, 6.0, ((0, 32), (1, 8))),
        "kept_blocks": draw_kept_blocks(jax.random.fold_in(splits[6], 71), 0),
        "kept_count": ragged(splits[5], SHARDS, KEPT, KEEP_MAX, 2).astype(jnp.int32),
    }


def attend(queries, keys, values):
    row_count = queries.shape[0]
    group_size = QH // KVH

    def one_head(head_index):
        query_block = lax.dynamic_slice_in_dim(queries, head_index * group_size * HD, group_size * HD, 1)
        query_block = query_block.reshape(row_count * group_size, HD)
        key_part = lax.dynamic_index_in_dim(keys, head_index, 1, keepdims=False)
        value_part = lax.dynamic_index_in_dim(values, head_index, 1, keepdims=False)
        scores = jnp.dot(query_block, key_part.T, preferred_element_type=jnp.float32) * (QPS ** -0.5)
        row_top = jnp.max(scores, axis=1, keepdims=True)
        weights = jnp.exp(scores - row_top)
        row_total = jnp.sum(weights, axis=1, keepdims=True)
        summed = jnp.dot(weights.astype(jnp.bfloat16), value_part, preferred_element_type=jnp.float32)
        return (summed / row_total).reshape(row_count, group_size * HD)

    per_head = lax.map(one_head, jnp.arange(KVH, dtype=jnp.int32))
    return per_head.transpose(1, 0, 2).reshape(row_count, QH * HD).astype(jnp.bfloat16)


def reference(q_first, q_second, k_cache, v_cache, kept_blocks, kept_count):
    out_first = attend(q_first, k_cache, v_cache)
    offsets = (jnp.cumsum(kept_count) - kept_count).astype(jnp.int32)
    slot_ids = jnp.arange(KEEP_MAX, dtype=jnp.int32)
    target = jnp.where(slot_ids[None, :] < kept_count[:, None], offsets[:, None] + slot_ids[None, :], KEPT).astype(jnp.int32)
    global_block = (jnp.arange(SHARDS, dtype=jnp.int32)[:, None] * BLK_DEV + kept_blocks).astype(jnp.int32)
    block_order = jnp.zeros((KEPT,), jnp.int32).at[target.reshape(-1)].set(global_block.reshape(-1), mode="drop")
    key_blocks = k_cache.reshape(SHARDS * BLK_DEV, BLK, KVH, HD)[block_order].reshape(KEPT * BLK, KVH, HD)
    value_blocks = v_cache.reshape(SHARDS * BLK_DEV, BLK, KVH, HD)[block_order].reshape(KEPT * BLK, KVH, HD)
    out_second = attend(q_second, key_blocks, value_blocks)
    return (out_first, out_second)
```

```python
import functools

import jax
import jax.numpy as jnp
from jax import lax
from jax.experimental import pallas as pl
from jax.experimental.pallas import tpu as pltpu
from jax.sharding import PartitionSpec as P

HD = 128
BLK = 128
F32 = jnp.float32
BF16 = jnp.bfloat16
SCALE = 168 ** -0.5 * 1.4426950408889634
NEG = -1e30
MESH = pl.DeviceIdType.MESH

KV = 2
KEYS = 4096
ROWS = 1536
QT = 256
TILES = ROWS // QT
CK = 1024
NB = KEYS // CK
NX, NY, NZ = 4, 4, 8
GRP = ROWS // NY
OWN = GRP // NZ
VROWS = HD + 16

Q_HOPS = ((0, 1), (1, 0), (1, 1), (3, 0), (3, 1), (2, 0), (2, 1))


def head_at(me, dx, dc):
    x, c = me // 2, me % 2
    return ((x + dx) % NX) * 2 + (c + dc) % 2


def ctx_at(y, z):
    return (y % NY) * NZ + z % NZ


def remote(src, dst, send_sem, recv_sem, **where):
    return pltpu.make_async_remote_copy(
        src_ref=src, dst_ref=dst, send_sem=send_sem, recv_sem=recv_sem, device_id=where, device_id_type=MESH
    )


def prep_keys(kraw, kx, stage):
    n = stage.shape[0]

    def step(i, c):
        stage[...] = kraw[pl.ds(i * n, n), :].astype(F32)
        for h in range(KV):
            k = stage[pl.ds(h, n // 2, stride=2), :].astype(BF16)
            rows = pl.ds(i * (n // 2), n // 2)
            kx[h, rows, 0:HD] = k
            kx[h, rows, HD : 2 * HD] = k
        return c

    lax.fori_loop(0, KEYS * KV // n, step, 0)


def prep_values(vraw, vt, stage):
    n = stage.shape[0]

    def step(i, c):
        stage[...] = vraw[pl.ds(i * n, n), :].astype(F32)
        for h in range(KV):
            v = stage[pl.ds(h, n // 2, stride=2), :].astype(BF16)
            vt[h, 0:HD, pl.ds(pl.multiple_of(i * (n // 2), n // 2), n // 2)] = v.T
        return c

    lax.fori_loop(0, KEYS * KV // n, step, 0)
    for h in range(KV):
        vt[h, HD:VROWS, :] = jnp.ones((VROWS - HD, KEYS), BF16)


def prep_queries(qraw, qx, blk, place):
    def step(hs, c):
        x = qraw[blk, hs].astype(F32) * SCALE
        rows = pl.ds(pl.multiple_of(place(hs) * (4 * OWN), 64), 4 * OWN)
        for h in range(KV):
            a = x[:, h * 256 : h * 256 + 128]
            b = x[:, h * 256 + 128 : h * 256 + 256]
            pieces = []
            for j in range(4):
                pieces += [a[j * 24 : j * 24 + 24], b[j * 24 : j * 24 + 24]]
            full = jnp.concatenate(pieces, axis=0)
            hi = full.astype(BF16)
            qx[blk, h, rows, 0:HD] = hi
            qx[blk, h, rows, HD : 2 * HD] = (full - hi.astype(F32)).astype(BF16)
        return c

    lax.fori_loop(0, 8, step, 0)


def scores_step(i, q, kx, h, s_ref, bias, blk, top):
    s = lax.dot_general(
        kx[h, pl.ds(i * CK, CK), :], q, (((1,), (1,)), ((), ())), preferred_element_type=F32
    )
    s_ref[pl.ds(i * CK, CK), :] = s
    for b in range(CK // BLK):
        part = s[b * BLK : (b + 1) * BLK].reshape(BLK // 8, 8, QT)
        top = jnp.maximum(top, jnp.max(part, axis=0) + bias[blk, pl.ds(i * (CK // BLK) + b, 1), :])
    return top


def values_step(i, vt, h, s_ref, bias, blk, top, total):
    pieces = []
    for b in range(CK // BLK):
        shift = top - bias[blk, pl.ds(i * (CK // BLK) + b, 1), :]
        pieces.append(jnp.exp2(s_ref[pl.ds(i * CK + b * BLK, BLK), :] - shift).astype(BF16))
    p = jnp.concatenate(pieces, axis=0)
    d = lax.dot_general(
        vt[h, :, pl.ds(i * CK, CK)], p, (((1,), (0,)), ((), ())), preferred_element_type=F32
    )
    return d if total is None else total + d


def sweep(blk, kx, vt, qx, bias, obuf, lse, s0, s1):
    n = KV * TILES

    def q_tile(t):
        return qx[blk, t // TILES, pl.ds(pl.multiple_of((t % TILES) * QT, QT), QT), :]

    def first(t, s):
        q = q_tile(t)
        top = jnp.full((8, QT), NEG, F32)
        for i in range(NB):
            top = scores_step(i, q, kx, t // TILES, s, bias, blk, top)
        return jnp.max(top, axis=0, keepdims=True)

    def both(ta, sa, tb, sb, m):
        q = q_tile(ta)
        top = jnp.full((8, QT), NEG, F32)
        total = None
        for i in range(NB):
            top = scores_step(i, q, kx, ta // TILES, sa, bias, blk, top)
            total = values_step(i, vt, tb // TILES, sb, bias, blk, m, total)
        norm = total[HD : HD + 1, :]
        h, cols = tb // TILES, pl.ds(pl.multiple_of((tb % TILES) * QT, QT), QT)
        obuf[blk, h, cols, :] = (total[0:HD, :] * (1.0 / norm)).T.astype(BF16)
        lse[blk, h, :, cols] = m + jnp.log2(norm)
        return jnp.max(top, axis=0, keepdims=True)

    def step(i, m):
        m = both(2 * i + 1, s1, 2 * i, s0, m)
        return both(jnp.minimum(2 * i + 2, n - 1), s0, 2 * i + 1, s1, m)

    lax.fori_loop(0, n // 2, step, first(0, s0))


def combine_y(blk, obuf, lse, r1, l1, c1, lz):
    rows = []
    for h in range(KV):
        ls = [lse[blk, h, :, 0:GRP]] + [l1[blk, k, h] for k in range(NY - 1)]
        m = functools.reduce(jnp.maximum, ls)
        ws = [jnp.exp2(l - m) for l in ls]
        total = functools.reduce(jnp.add, ws)
        rows += [w / total for w in ws]
        both = m + jnp.log2(total)
        for z in range(NZ):
            lz[blk, z, h : h + 1, 0:OWN] = both[:, z * OWN : (z + 1) * OWN]
    w = jnp.concatenate(rows, axis=0).T
    for h in range(KV):
        acc = obuf[blk, h, 0:GRP, :].astype(F32) * w[:, h * NY : h * NY + 1]
        for k in range(NY - 1):
            acc += r1[blk, k, h].astype(F32) * w[:, h * NY + k + 1 : h * NY + k + 2]
        c1[blk, h] = acc.astype(BF16)


def combine_z(blk, z, c1, lz, r2, l2, out_ref):
    mine = pl.ds(pl.multiple_of(z * OWN, 16), OWN)
    ls = [lz[blk, z]] + [l2[blk, j] for j in range(NZ - 1)]
    m = functools.reduce(jnp.maximum, ls)
    ws = [jnp.exp2(l - m) for l in ls]
    total = functools.reduce(jnp.add, ws)
    w = jnp.concatenate([x / total for x in ws], axis=0).T
    for h in range(KV):
        acc = c1[blk, h, mine, :].astype(F32) * w[0:OWN, h : h + 1]
        for j in range(NZ - 1):
            col = (j + 1) * KV + h
            acc += r2[blk, j, h].astype(F32) * w[0:OWN, col : col + 1]
        for g in range(2):
            at = (h * 2 + g) * HD
            out_ref[:, at : at + HD] = acc[g * 24 : (g + 1) * 24].astype(BF16)


def kernel(
    q0, q1, k_hbm, v_hbm, kept_ref, count_ref, out0, out1,
    kraw, vraw, qraw, kx, vt, stage, qx, bias, s0, s1, obuf, lse, r1, l1, c1, lz, r2, l2,
    local, qs_sem, qr_sem, ys_sem, yr_sem, yls_sem, ylr_sem, zs_sem, zr_sem, zls_sem, zlr_sem,
):
    me, ctx = lax.axis_index("head"), lax.axis_index("ctx")
    y, z = ctx // NZ, ctx % NZ
    outs = (out0, out1)
    kcopy = pltpu.make_async_copy(k_hbm, kraw, local.at[0])
    vcopy = pltpu.make_async_copy(v_hbm, vraw, local.at[1])
    kcopy.start()
    vcopy.start()
    own = []
    cols = pl.ds(pl.multiple_of(me * 512, 512), 512)
    for blk, q in enumerate((q0, q1)):
        own.append(pltpu.make_async_copy(q.at[:, cols], qraw.at[blk, me], local.at[2 + blk]))
        own[-1].start()

    barrier = pltpu.get_barrier_semaphore()
    for dx, dc in Q_HOPS:
        pl.semaphore_signal(barrier, inc=1, device_id={"head": head_at(me, dx, dc)}, device_id_type=MESH)
    for k in range(1, NY):
        pl.semaphore_signal(barrier, inc=1, device_id={"ctx": ctx_at(y + k, z)}, device_id_type=MESH)
    for j in range(1, NZ):
        pl.semaphore_signal(barrier, inc=1, device_id={"ctx": ctx_at(y, z + j)}, device_id_type=MESH)
    pl.semaphore_wait(barrier, len(Q_HOPS) + NY - 1 + NZ - 1)

    sends = []

    def q_copy(blk, n, dest, source):
        to = pl.ds(pl.multiple_of(dest * 512, 512), 512)
        return remote(
            (q0, q1)[blk].at[:, to], qraw.at[blk, source], qs_sem.at[blk, n], qr_sem.at[blk, n], head=dest
        )

    for blk in range(2):
        for n, (dx, dc) in enumerate(Q_HOPS):
            copy = q_copy(blk, n, head_at(me, dx, dc), me)
            copy.start()
            sends.append(copy)

    def wait_queries(blk):
        own[blk].wait()
        for n, (dx, dc) in enumerate(Q_HOPS):
            q_copy(blk, n, me, head_at(me, NX - dx, dc)).wait_recv()

    flags = jnp.where(
        (kept_ref[...] == lax.broadcasted_iota(jnp.int32, (32, 32), 0))
        & (lax.broadcasted_iota(jnp.int32, (32, 32), 1) < count_ref[0]),
        1.0, 0.0,
    )
    kept = jnp.max(flags, axis=1, keepdims=True)
    bias[0] = jnp.zeros((32, QT), F32)
    bias[1] = jnp.broadcast_to((1.0 - kept) * NEG, (32, QT))
    lz[...] = jnp.zeros(lz.shape, F32)

    kcopy.wait()
    prep_keys(kraw, kx, stage)
    vcopy.wait()
    prep_values(vraw, vt, stage)

    def place(hs):
        return ((hs // 2 + NY - y) % NY) * 2 + hs % 2

    def y_copies(blk):
        made = []
        for k in range(1, NY):
            at = pl.ds(k * GRP, GRP)
            dest = ctx_at(y + k, z)
            made.append(remote(
                obuf.at[blk, :, at, :], r1.at[blk, k - 1], ys_sem.at[blk, k - 1], yr_sem.at[blk, k - 1], ctx=dest
            ))
            made.append(remote(
                lse.at[blk, :, :, at], l1.at[blk, k - 1], yls_sem.at[blk, k - 1], ylr_sem.at[blk, k - 1], ctx=dest
            ))
        return made

    def z_copies(blk):
        made = []
        for j in range(1, NZ):
            to = (z + j) % NZ
            at = pl.ds(pl.multiple_of(to * OWN, 16), OWN)
            dest = ctx_at(y, to)
            made.append(remote(
                c1.at[blk, :, at, :], r2.at[blk, j - 1], zs_sem.at[blk, j - 1], zr_sem.at[blk, j - 1], ctx=dest
            ))
            made.append(remote(
                lz.at[blk, to], l2.at[blk, j - 1], zls_sem.at[blk, j - 1], zlr_sem.at[blk, j - 1], ctx=dest
            ))
        return made

    def begin(copies):
        for copy in copies:
            copy.start()
        sends.extend(copies)
        return copies

    def arrive(copies):
        for copy in copies:
            copy.wait_recv()

    wait_queries(0)
    prep_queries(qraw, qx, 0, place)
    sweep(0, kx, vt, qx, bias, obuf, lse, s0, s1)
    ya = begin(y_copies(0))
    wait_queries(1)
    prep_queries(qraw, qx, 1, place)
    sweep(1, kx, vt, qx, bias, obuf, lse, s0, s1)
    yb = begin(y_copies(1))
    arrive(ya)
    combine_y(0, obuf, lse, r1, l1, c1, lz)
    za = begin(z_copies(0))
    arrive(yb)
    combine_y(1, obuf, lse, r1, l1, c1, lz)
    zb = begin(z_copies(1))
    arrive(za)
    combine_z(0, z, c1, lz, r2, l2, outs[0])
    arrive(zb)
    combine_z(1, z, c1, lz, r2, l2, outs[1])
    for copy in sends:
        copy.wait_send()


def shards(q_first, q_second, k_cache, v_cache, kept_blocks, kept_count):
    anyspace = pl.BlockSpec(memory_space=pl.ANY)
    vmem = pl.BlockSpec(memory_space=pltpu.VMEM)
    dma = pltpu.SemaphoreType.DMA
    out = jax.ShapeDtypeStruct((24, 512), BF16)
    return pl.pallas_call(
        kernel,
        out_shape=(out, out),
        in_specs=[anyspace] * 4 + [vmem, pl.BlockSpec(memory_space=pltpu.SMEM)],
        out_specs=(vmem, vmem),
        scratch_shapes=[
            pltpu.VMEM((KEYS * KV, HD), BF16),
            pltpu.VMEM((KEYS * KV, HD), BF16),
            pltpu.VMEM((2, 8, 96, 512), BF16),
            pltpu.VMEM((KV, KEYS, 2 * HD), BF16),
            pltpu.VMEM((KV, VROWS, KEYS), BF16),
            pltpu.VMEM((1024, HD), F32),
            pltpu.VMEM((2, KV, ROWS, 2 * HD), BF16),
            pltpu.VMEM((2, 32, QT), F32),
            pltpu.VMEM((KEYS, QT), F32),
            pltpu.VMEM((KEYS, QT), F32),
            pltpu.VMEM((2, KV, ROWS, HD), BF16),
            pltpu.VMEM((2, KV, 1, ROWS), F32),
            pltpu.VMEM((2, NY - 1, KV, GRP, HD), BF16),
            pltpu.VMEM((2, NY - 1, KV, 1, GRP), F32),
            pltpu.VMEM((2, KV, GRP, HD), BF16),
            pltpu.VMEM((2, NZ, KV, 128), F32),
            pltpu.VMEM((2, NZ - 1, KV, OWN, HD), BF16),
            pltpu.VMEM((2, NZ - 1, KV, 128), F32),
            dma((4,)),
            dma((2, 7)), dma((2, 7)),
            dma((2, 3)), dma((2, 3)), dma((2, 3)), dma((2, 3)),
            dma((2, 7)), dma((2, 7)), dma((2, 7)), dma((2, 7)),
        ],
        compiler_params=pltpu.CompilerParams(
            collective_id=0, has_side_effects=True, vmem_limit_bytes=60 * 1024 * 1024
        ),
    )(
        q_first, q_second,
        k_cache.reshape(KEYS * KV, HD), v_cache.reshape(KEYS * KV, HD),
        kept_blocks, kept_count,
    )


def solution(mesh):
    placed = (
        P("head", None),
        P("head", None),
        P("ctx", "head", None),
        P("ctx", "head", None),
        P("ctx", None),
        P("ctx"),
    )
    return jax.shard_map(
        shards,
        mesh=mesh,
        in_specs=placed,
        out_specs=(P("ctx", "head"), P("ctx", "head")),
        check_vma=False,
    )
```

```python
import functools

import jax
import jax.numpy as jnp
from jax import lax
from jax.experimental import pallas as pl
from jax.experimental.pallas import tpu as pltpu
from jax.sharding import PartitionSpec as P

HD = 128
BLK = 128
F32 = jnp.float32
BF16 = jnp.bfloat16
SCALE = 168 ** -0.5 * 1.4426950408889634
NEG = -1e30
MESH = pl.DeviceIdType.MESH

KV = 2
KEYS = 4096
ROWS = 1536
QT = 256
TILES = ROWS // QT
CK = 1024
NB = KEYS // CK
NX, NY, NZ = 4, 4, 8
GRP = ROWS // NY
OWN = GRP // NZ
VROWS = HD + 16

Q_HOPS = ((0, 1), (1, 0), (1, 1), (3, 0), (3, 1), (2, 0), (2, 1))


def head_at(me, dx, dc):
    x, c = me // 2, me % 2
    return ((x + dx) % NX) * 2 + (c + dc) % 2


def ctx_at(y, z):
    return (y % NY) * NZ + z % NZ


def remote(src, dst, send_sem, recv_sem, **where):
    return pltpu.make_async_remote_copy(
        src_ref=src, dst_ref=dst, send_sem=send_sem, recv_sem=recv_sem, device_id=where, device_id_type=MESH
    )


def prep_keys(kraw, kx, stage):
    n = stage.shape[0]

    def step(i, c):
        stage[...] = kraw[pl.ds(i * n, n), :].astype(F32)
        for h in range(KV):
            k = stage[pl.ds(h, n // 2, stride=2), :].astype(BF16)
            rows = pl.ds(i * (n // 2), n // 2)
            kx[h, rows, 0:HD] = k
            kx[h, rows, HD : 2 * HD] = k
        return c

    lax.fori_loop(0, KEYS * KV // n, step, 0)


def prep_values(vraw, vt, stage):
    n = stage.shape[0]

    def step(i, c):
        stage[...] = vraw[pl.ds(i * n, n), :].astype(F32)
        for h in range(KV):
            v = stage[pl.ds(h, n // 2, stride=2), :].astype(BF16)
            vt[h, 0:HD, pl.ds(pl.multiple_of(i * (n // 2), n // 2), n // 2)] = v.T
        return c

    lax.fori_loop(0, KEYS * KV // n, step, 0)
    for h in range(KV):
        vt[h, HD:VROWS, :] = jnp.ones((VROWS - HD, KEYS), BF16)


def prep_queries(qraw, qx, blk, hs, pos):
    x = qraw[blk, hs].astype(F32) * SCALE
    rows = pl.ds(pl.multiple_of(pos * (4 * OWN), 64), 4 * OWN)
    for h in range(KV):
        a = x[:, h * 256 : h * 256 + 128]
        b = x[:, h * 256 + 128 : h * 256 + 256]
        pieces = []
        for j in range(4):
            pieces += [a[j * 24 : j * 24 + 24], b[j * 24 : j * 24 + 24]]
        full = jnp.concatenate(pieces, axis=0)
        hi = full.astype(BF16)
        qx[blk, h, rows, 0:HD] = hi
        qx[blk, h, rows, HD : 2 * HD] = (full - hi.astype(F32)).astype(BF16)


def scores_step(i, q, kx, h, s_ref, bias, blk, top):
    s = lax.dot_general(
        kx[h, pl.ds(i * CK, CK), :], q, (((1,), (1,)), ((), ())), preferred_element_type=F32
    )
    s_ref[pl.ds(i * CK, CK), :] = s
    for b in range(CK // BLK):
        part = s[b * BLK : (b + 1) * BLK].reshape(BLK // 8, 8, QT)
        top = jnp.maximum(top, jnp.max(part, axis=0) + bias[blk, pl.ds(i * (CK // BLK) + b, 1), :])
    return top


def values_step(i, vt, h, s_ref, bias, blk, top, total):
    pieces = []
    for b in range(CK // BLK):
        shift = top - bias[blk, pl.ds(i * (CK // BLK) + b, 1), :]
        pieces.append(jnp.exp2(s_ref[pl.ds(i * CK + b * BLK, BLK), :] - shift).astype(BF16))
    p = jnp.concatenate(pieces, axis=0)
    d = lax.dot_general(
        vt[h, :, pl.ds(i * CK, CK)], p, (((1,), (0,)), ((), ())), preferred_element_type=F32
    )
    return d if total is None else total + d


def make_tiles(kx, vt, qx, bias, obuf, lse, s0, s1):
    slots = (s0, s1)

    def cols(i):
        return pl.ds(pl.multiple_of((i % TILES) * QT, QT), QT)

    def finish(i, h, total, m):
        norm = total[HD : HD + 1, :]
        obuf[i // TILES, h, cols(i), :] = (total[0:HD, :] * (1.0 / norm)).T.astype(BF16)
        lse[i // TILES, h, :, cols(i)] = m + jnp.log2(norm)

    def run(score=None, value=None, m=None):
        top = jnp.full((8, QT), NEG, F32)
        total = None
        if score is not None:
            ia, ha = score
            q = qx[ia // TILES, ha, cols(ia), :]
        for n in range(NB):
            if score is not None:
                top = scores_step(n, q, kx, ha, slots[ha], bias, ia // TILES, top)
            if value is not None:
                ib, hb = value
                total = values_step(n, vt, hb, slots[hb], bias, ib // TILES, m, total)
        if value is not None:
            finish(ib, hb, total, m)
        return jnp.max(top, axis=0, keepdims=True)

    return run


def combine_y(blk, h, mine, obuf, lse, r1, l1, c1, lz):
    ls = [lse[blk, h, :, mine]] + [l1[blk, k, h] for k in range(NY - 1)]
    m = functools.reduce(jnp.maximum, ls)
    ws = [jnp.exp2(l - m) for l in ls]
    total = functools.reduce(jnp.add, ws)
    both = m + jnp.log2(total)
    for z in range(NZ):
        lz[blk, z, h, :, 0:OWN] = both[:, z * OWN : (z + 1) * OWN]
    w = jnp.concatenate([w / total for w in ws] * 2, axis=0).T
    acc = obuf[blk, h, mine, :].astype(F32) * w[:, 0:1]
    for k in range(NY - 1):
        acc += r1[blk, k, h].astype(F32) * w[:, k + 1 : k + 2]
    c1[blk, h] = acc.astype(BF16)


def combine_z(blk, h, z, c1, lz, r2, l2, out_ref):
    mine = pl.ds(pl.multiple_of(z * OWN, 16), OWN)
    ls = [lz[blk, z, h]] + [l2[blk, j, h] for j in range(NZ - 1)]
    m = functools.reduce(jnp.maximum, ls)
    ws = [jnp.exp2(l - m) for l in ls]
    total = functools.reduce(jnp.add, ws)
    w = jnp.concatenate([x / total for x in ws], axis=0).T
    acc = c1[blk, h, mine, :].astype(F32) * w[0:OWN, 0:1]
    for j in range(NZ - 1):
        acc += r2[blk, j, h].astype(F32) * w[0:OWN, j + 1 : j + 2]
    for g in range(2):
        at = (h * 2 + g) * HD
        out_ref[blk, :, at : at + HD] = acc[g * 24 : (g + 1) * 24].astype(BF16)


def kernel(
    q0, q1, k_hbm, v_hbm, kept_ref, count_ref, out,
    kraw, vraw, qraw, kx, vt, stage, qx, bias, s0, s1, obuf, lse, r1, l1, c1, lz, r2, l2,
    local, qs_sem, qr_sem, ys_sem, yr_sem, yls_sem, ylr_sem, zs_sem, zr_sem, zls_sem, zlr_sem, near, far,
):
    me, ctx = lax.axis_index("head"), lax.axis_index("ctx")
    x, y, z = me // 2, ctx // NZ, ctx % NZ

    barrier = pltpu.get_barrier_semaphore()
    for dx, dc in Q_HOPS:
        pl.semaphore_signal(barrier, inc=1, device_id={"head": head_at(me, dx, dc)}, device_id_type=MESH)
    for k in range(1, NY):
        pl.semaphore_signal(barrier, inc=1, device_id={"ctx": ctx_at(y + k, z)}, device_id_type=MESH)
    for j in (1, NZ - 1):
        pl.semaphore_signal(barrier, inc=1, device_id={"ctx": ctx_at(y, z + j)}, device_id_type=MESH)

    kcopy = pltpu.make_async_copy(k_hbm, kraw, local.at[0])
    vcopy = pltpu.make_async_copy(v_hbm, vraw, local.at[1])
    own = []
    cols = pl.ds(pl.multiple_of(me * 512, 512), 512)
    for blk, q in enumerate((q0, q1)):
        own.append(pltpu.make_async_copy(q.at[:, cols], qraw.at[blk, me], local.at[2 + blk]))
    own[0].start()
    kcopy.start()
    vcopy.start()
    own[1].start()

    pl.semaphore_wait(barrier, len(Q_HOPS) + NY - 1 + 2)

    sends = []

    def q_copy(blk, n, dest, source):
        to = pl.ds(pl.multiple_of(dest * 512, 512), 512)
        return remote(
            (q0, q1)[blk].at[:, to], qraw.at[blk, source], qs_sem.at[blk, n], qr_sem.at[blk, n], head=dest
        )

    for blk in range(2):
        for n, (dx, dc) in enumerate(Q_HOPS):
            copy = q_copy(blk, n, head_at(me, dx, dc), me)
            copy.start()
            sends.append(copy)
    for j in (1, NZ - 1):
        pl.semaphore_signal(near, inc=1, device_id={"ctx": ctx_at(y, z + j)}, device_id_type=MESH)

    flags = jnp.where(
        (kept_ref[...] == lax.broadcasted_iota(jnp.int32, (32, 32), 0))
        & (lax.broadcasted_iota(jnp.int32, (32, 32), 1) < count_ref[0]),
        1.0, 0.0,
    )
    kept = jnp.max(flags, axis=1, keepdims=True)
    bias[0] = jnp.zeros((32, QT), F32)
    bias[1] = jnp.broadcast_to((1.0 - kept) * NEG, (32, QT))
    lz[...] = jnp.zeros(lz.shape, F32)

    kcopy.wait()
    prep_keys(kraw, kx, stage)
    vcopy.wait()
    prep_values(vraw, vt, stage)

    pl.semaphore_wait(near, 2)
    for j in (2, NZ - 2):
        pl.semaphore_signal(far, inc=1, device_id={"ctx": ctx_at(y, z + j)}, device_id_type=MESH)

    def arrived(blk, hops):
        for n, (dx, dc) in enumerate(Q_HOPS):
            if dx in hops:
                q_copy(blk, n, me, head_at(me, NX - dx, dc)).wait_recv()

    swap = (3 - (x + NX - y) % NX) // 3

    def spot(blk, chip):
        r = (chip + NX - (x, y)[blk]) % NX
        b1, b0 = r // 2, r % 2
        if blk == 0:
            return 2 * b1 + (b0 + b1) % 2
        high = 1 - (b0 + b1) % 2
        return 2 * high + (1 - b1 + swap * (1 - high)) % 2

    def prepare(blk, chip):
        for c in range(2):
            prep_queries(qraw, qx, blk, chip * 2 + c, spot(blk, chip) * 2 + c)

    def y_copy(blk, h, k, at):
        dest = ctx_at(y + k, z)
        at = pl.ds(pl.multiple_of(at * GRP, GRP), GRP)
        return (
            remote(obuf.at[blk, h, at, :], r1.at[blk, k - 1, h],
                   ys_sem.at[blk, h, k - 1], yr_sem.at[blk, h, k - 1], ctx=dest),
            remote(lse.at[blk, h, :, at], l1.at[blk, k - 1, h],
                   yls_sem.at[blk, h, k - 1], ylr_sem.at[blk, h, k - 1], ctx=dest),
        )

    def y_send(blk, h, p):
        if blk == 0:
            k = (x + (0, 1, 3, 2)[p] + NY - y) % NY

            @pl.when(k > 0)
            def _():
                for copy in y_copy(0, h, k, p):
                    copy.start()
        else:
            for copy in y_copy(1, h, (2 - swap, 1 + swap, 3)[p], p):
                copy.start()

    def y_arrive(blk, h):
        for k in range(1, NY):
            for copy in y_copy(blk, h, k, 0):
                copy.wait_recv()

    def z_copy(blk, h, j):
        to = (z + j) % NZ
        at = pl.ds(pl.multiple_of(to * OWN, 16), OWN)
        dest = ctx_at(y, to)
        return (
            remote(c1.at[blk, h, at, :], r2.at[blk, j - 1, h],
                   zs_sem.at[blk, h, j - 1], zr_sem.at[blk, h, j - 1], ctx=dest),
            remote(lz.at[blk, to, h], l2.at[blk, j - 1, h],
                   zls_sem.at[blk, h, j - 1], zlr_sem.at[blk, h, j - 1], ctx=dest),
        )

    def merge_y(blk, h):
        mine = pl.ds(pl.multiple_of(spot(blk, y) * GRP, GRP), GRP)
        y_arrive(blk, h)
        combine_y(blk, h, mine, obuf, lse, r1, l1, c1, lz)
        for j in (4, 3, 5, 2, 6, 1, 7):
            for copy in z_copy(blk, h, j):
                copy.start()

    def merge_z(blk, h):
        for j in range(1, NZ):
            for copy in z_copy(blk, h, j):
                copy.wait_recv()
        combine_z(blk, h, z, c1, lz, r2, l2, out)

    tile = make_tiles(kx, vt, qx, bias, obuf, lse, s0, s1)
    own[0].wait()
    arrived(0, (0,))
    prepare(0, x)
    m = tile(score=(0, 0))
    m = tile(score=(0, 1), value=(0, 0), m=m)

    def step(i, m):
        @pl.when(i == 0)
        def _():
            arrived(0, (1, 3))
            prepare(0, (x + 3) % NX)
            prepare(0, (x + 1) % NX)

        @pl.when(i == 3)
        def _():
            arrived(0, (2,))
            prepare(0, (x + 2) % NX)

        @pl.when(i == 5)
        def _():
            own[1].wait()
            arrived(1, (0, 1, 3))
            for d in (0, 1, 3):
                prepare(1, (x + d) % NX)

        @pl.when(i == 6)
        def _():
            arrived(1, (2,))
            prepare(1, (x + 2) % NX)

        for blk, h, p, when in (
            (0, 0, 0, 1), (0, 1, 0, 2), (0, 0, 1, 2), (0, 1, 1, 3), (0, 0, 2, 4), (0, 1, 2, 5), (0, 0, 3, 5), (0, 1, 3, 6),
            (1, 0, 0, 7), (1, 1, 0, 8), (1, 0, 1, 8), (1, 1, 1, 9),
        ):
            @pl.when(i == when)
            def _():
                y_send(blk, h, p)

        m = tile(score=(i + 1, 0), value=(i, 1), m=m)
        return tile(score=(i + 1, 1), value=(i + 1, 0), m=m)

    last = 2 * TILES - 1
    m = lax.fori_loop(0, last - 1, step, m)
    y_send(1, 0, 2)
    pl.semaphore_wait(far, 2)
    merge_y(0, 0)
    merge_y(0, 1)
    m = tile(score=(last, 0), value=(last - 1, 1), m=m)
    y_send(1, 1, 2)
    m = tile(score=(last, 1), value=(last, 0), m=m)
    tile(value=(last, 1), m=m)
    merge_y(1, 0)
    merge_y(1, 1)
    for blk in range(2):
        for h in range(KV):
            merge_z(blk, h)
    for copy in sends:
        copy.wait_send()
    for blk in range(2):
        for h in range(KV):
            for k in range(1, NY):
                for copy in y_copy(blk, h, k, 0):
                    copy.wait_send()
            for j in range(1, NZ):
                for copy in z_copy(blk, h, j):
                    copy.wait_send()


def shards(q_first, q_second, k_cache, v_cache, kept_blocks, kept_count):
    anyspace = pl.BlockSpec(memory_space=pl.ANY)
    vmem = pl.BlockSpec(memory_space=pltpu.VMEM)
    dma = pltpu.SemaphoreType.DMA
    both = pl.pallas_call(
        kernel,
        out_shape=jax.ShapeDtypeStruct((2, 24, 512), BF16),
        in_specs=[anyspace] * 4 + [vmem, pl.BlockSpec(memory_space=pltpu.SMEM)],
        out_specs=vmem,
        scratch_shapes=[
            pltpu.VMEM((KEYS * KV, HD), BF16),
            pltpu.VMEM((KEYS * KV, HD), BF16),
            pltpu.VMEM((2, 8, 96, 512), BF16),
            pltpu.VMEM((KV, KEYS, 2 * HD), BF16),
            pltpu.VMEM((KV, VROWS, KEYS), BF16),
            pltpu.VMEM((1024, HD), F32),
            pltpu.VMEM((2, KV, ROWS, 2 * HD), BF16),
            pltpu.VMEM((2, 32, QT), F32),
            pltpu.VMEM((KEYS, QT), F32),
            pltpu.VMEM((KEYS, QT), F32),
            pltpu.VMEM((2, KV, ROWS, HD), BF16),
            pltpu.VMEM((2, KV, 1, ROWS), F32),
            pltpu.VMEM((2, NY - 1, KV, GRP, HD), BF16),
            pltpu.VMEM((2, NY - 1, KV, 1, GRP), F32),
            pltpu.VMEM((2, KV, GRP, HD), BF16),
            pltpu.VMEM((2, NZ, KV, 1, 128), F32),
            pltpu.VMEM((2, NZ - 1, KV, OWN, HD), BF16),
            pltpu.VMEM((2, NZ - 1, KV, 1, 128), F32),
            dma((4,)),
            dma((2, 7)), dma((2, 7)),
            dma((2, KV, 3)), dma((2, KV, 3)), dma((2, KV, 3)), dma((2, KV, 3)),
            dma((2, KV, 7)), dma((2, KV, 7)), dma((2, KV, 7)), dma((2, KV, 7)),
            pltpu.SemaphoreType.REGULAR, pltpu.SemaphoreType.REGULAR,
        ],
        compiler_params=pltpu.CompilerParams(
            collective_id=0, has_side_effects=True, vmem_limit_bytes=60 * 1024 * 1024
        ),
    )(
        q_first, q_second,
        k_cache.reshape(KEYS * KV, HD), v_cache.reshape(KEYS * KV, HD),
        kept_blocks, kept_count,
    )
    return both[0], both[1]


def solution(mesh):
    placed = (
        P("head", None),
        P("head", None),
        P("ctx", "head", None),
        P("ctx", "head", None),
        P("ctx", None),
        P("ctx"),
    )
    return jax.shard_map(
        shards,
        mesh=mesh,
        in_specs=placed,
        out_specs=(P("ctx", "head"), P("ctx", "head")),
        check_vma=False,
    )
```

```python
import functools

import jax
import jax.numpy as jnp
from jax import lax
from jax.experimental import pallas as pl
from jax.experimental.pallas import tpu as pltpu
from jax.sharding import PartitionSpec as P

HD = 128
BLK = 128
F32 = jnp.float32
BF16 = jnp.bfloat16
SCALE = 168 ** -0.5 * 1.4426950408889634
NEG = -1e30
MESH = pl.DeviceIdType.MESH

KV = 2
KEYS = 4096
ROWS = 1536
QT = 256
TILES = ROWS // QT
CK = 1024
NB = KEYS // CK
NX, NY, NZ = 4, 4, 8
GRP = ROWS // NY
OWN = GRP // NZ
VROWS = HD + 16

Q_HOPS = ((0, 1), (1, 0), (1, 1), (3, 0), (3, 1), (2, 0), (2, 1))


def head_at(me, dx, dc):
    x, c = me // 2, me % 2
    return ((x + dx) % NX) * 2 + (c + dc) % 2


def ctx_at(y, z):
    return (y % NY) * NZ + z % NZ


def remote(src, dst, send_sem, recv_sem, **where):
    return pltpu.make_async_remote_copy(
        src_ref=src, dst_ref=dst, send_sem=send_sem, recv_sem=recv_sem, device_id=where, device_id_type=MESH
    )


def prep_keys(kraw, kx, stage):
    n = stage.shape[0]

    def step(i, c):
        stage[...] = kraw[pl.ds(i * n, n), :].astype(F32)
        for h in range(KV):
            k = stage[pl.ds(h, n // 2, stride=2), :].astype(BF16)
            rows = pl.ds(i * (n // 2), n // 2)
            kx[h, rows, 0:HD] = k
            kx[h, rows, HD : 2 * HD] = k
        return c

    lax.fori_loop(0, KEYS * KV // n, step, 0)


def prep_values(vraw, vt, stage):
    n = stage.shape[0]

    def step(i, c):
        stage[...] = vraw[pl.ds(i * n, n), :].astype(F32)
        for h in range(KV):
            v = stage[pl.ds(h, n // 2, stride=2), :].astype(BF16)
            vt[h, 0:HD, pl.ds(pl.multiple_of(i * (n // 2), n // 2), n // 2)] = v.T
        return c

    lax.fori_loop(0, KEYS * KV // n, step, 0)
    for h in range(KV):
        vt[h, HD:VROWS, :] = jnp.ones((VROWS - HD, KEYS), BF16)


def prep_queries(qraw, qx, blk, hs, pos):
    x = qraw[blk, hs].astype(F32) * SCALE
    rows = pl.ds(pl.multiple_of(pos * (4 * OWN), 64), 4 * OWN)
    for h in range(KV):
        a = x[:, h * 256 : h * 256 + 128]
        b = x[:, h * 256 + 128 : h * 256 + 256]
        pieces = []
        for j in range(4):
            pieces += [a[j * 24 : j * 24 + 24], b[j * 24 : j * 24 + 24]]
        full = jnp.concatenate(pieces, axis=0)
        hi = full.astype(BF16)
        qx[blk, h, rows, 0:HD] = hi
        qx[blk, h, rows, HD : 2 * HD] = (full - hi.astype(F32)).astype(BF16)


def scores_step(i, q, kx, h, s_ref, bias, blk, top):
    s = lax.dot_general(
        kx[h, pl.ds(i * CK, CK), :], q, (((1,), (1,)), ((), ())), preferred_element_type=F32
    )
    s_ref[pl.ds(i * CK, CK), :] = s
    for b in range(CK // BLK):
        part = s[b * BLK : (b + 1) * BLK].reshape(BLK // 8, 8, QT)
        top = jnp.maximum(top, jnp.max(part, axis=0) + bias[blk, pl.ds(i * (CK // BLK) + b, 1), :])
    return top


def values_step(i, vt, h, s_ref, bias, blk, top, total):
    pieces = []
    for b in range(CK // BLK):
        shift = top - bias[blk, pl.ds(i * (CK // BLK) + b, 1), :]
        pieces.append(jnp.exp2(s_ref[pl.ds(i * CK + b * BLK, BLK), :] - shift).astype(BF16))
    p = jnp.concatenate(pieces, axis=0)
    d = lax.dot_general(
        vt[h, :, pl.ds(i * CK, CK)], p, (((1,), (0,)), ((), ())), preferred_element_type=F32
    )
    return d if total is None else total + d


def make_tiles(kx, vt, qx, bias, obuf, lse, s0, s1):
    slots = (s0, s1)

    def cols(i):
        return pl.ds(pl.multiple_of((i % TILES) * QT, QT), QT)

    def finish(i, h, total, m):
        norm = total[HD : HD + 1, :]
        obuf[i // TILES, h, cols(i), :] = (total[0:HD, :] * (1.0 / norm)).T.astype(BF16)
        lse[i // TILES, h, :, cols(i)] = m + jnp.log2(norm)

    def run(score=None, value=None, m=None):
        top = jnp.full((8, QT), NEG, F32)
        total = None
        if score is not None:
            ia, ha = score
            q = qx[ia // TILES, ha, cols(ia), :]
        for n in range(NB):
            if score is not None:
                top = scores_step(n, q, kx, ha, slots[ha], bias, ia // TILES, top)
            if value is not None:
                ib, hb = value
                total = values_step(n, vt, hb, slots[hb], bias, ib // TILES, m, total)
        if value is not None:
            finish(ib, hb, total, m)
        return jnp.max(top, axis=0, keepdims=True)

    return run


def combine_y(blk, h, mine, obuf, lse, r1, l1, c1, lz):
    ls = [lse[blk, h, :, mine]] + [l1[blk, k, h] for k in range(NY - 1)]
    m = functools.reduce(jnp.maximum, ls)
    ws = [jnp.exp2(l - m) for l in ls]
    total = functools.reduce(jnp.add, ws)
    both = m + jnp.log2(total)
    for z in range(NZ):
        lz[blk, z, h, :, 0:OWN] = both[:, z * OWN : (z + 1) * OWN]
    w = jnp.concatenate([w / total for w in ws] * 2, axis=0).T
    acc = obuf[blk, h, mine, :].astype(F32) * w[:, 0:1]
    for k in range(NY - 1):
        acc += r1[blk, k, h].astype(F32) * w[:, k + 1 : k + 2]
    c1[blk, h] = acc.astype(BF16)


def combine_z(blk, h, z, c1, lz, r2, l2, out_ref):
    mine = pl.ds(pl.multiple_of(z * OWN, 16), OWN)
    ls = [lz[blk, z, h]] + [l2[blk, j, h] for j in range(NZ - 1)]
    m = functools.reduce(jnp.maximum, ls)
    ws = [jnp.exp2(l - m) for l in ls]
    total = functools.reduce(jnp.add, ws)
    w = jnp.concatenate([x / total for x in ws], axis=0).T
    acc = c1[blk, h, mine, :].astype(F32) * w[0:OWN, 0:1]
    for j in range(NZ - 1):
        acc += r2[blk, j, h].astype(F32) * w[0:OWN, j + 1 : j + 2]
    for g in range(2):
        at = (h * 2 + g) * HD
        out_ref[blk, :, at : at + HD] = acc[g * 24 : (g + 1) * 24].astype(BF16)


def kernel(
    q0, q1, k_hbm, v_hbm, kept_hbm, count_ref, out,
    kraw, vraw, qraw, kx, vt, stage, qx, bias, s0, s1, obuf, lse, r1, l1, c1, lz, r2, l2,
    local, qs_sem, qr_sem, ys_sem, yr_sem, yls_sem, ylr_sem, zs_sem, zr_sem, zls_sem, zlr_sem, near, far, kept_ref,
):
    me, ctx = lax.axis_index("head"), lax.axis_index("ctx")
    x, y, z = me // 2, ctx // NZ, ctx % NZ

    barrier = pltpu.get_barrier_semaphore()
    for dx, dc in Q_HOPS:
        pl.semaphore_signal(barrier, inc=1, device_id={"head": head_at(me, dx, dc)}, device_id_type=MESH)
    for k in range(1, NY):
        pl.semaphore_signal(barrier, inc=1, device_id={"ctx": ctx_at(y + k, z)}, device_id_type=MESH)
    for j in (1, NZ - 1):
        pl.semaphore_signal(barrier, inc=1, device_id={"ctx": ctx_at(y, z + j)}, device_id_type=MESH)

    kcopy = pltpu.make_async_copy(k_hbm, kraw, local.at[0])
    vcopy = pltpu.make_async_copy(v_hbm, vraw, local.at[1])
    own = []
    cols = pl.ds(pl.multiple_of(me * 512, 512), 512)
    for blk, q in enumerate((q0, q1)):
        own.append(pltpu.make_async_copy(q.at[:, cols], qraw.at[blk, me], local.at[2 + blk]))
    kept_copy = pltpu.make_async_copy(kept_hbm, kept_ref, local.at[4])
    own[0].start()
    kept_copy.start()
    kcopy.start()
    vcopy.start()
    own[1].start()

    pl.semaphore_wait(barrier, len(Q_HOPS) + NY - 1 + 2)

    sends = []

    def q_copy(blk, n, dest, source):
        to = pl.ds(pl.multiple_of(dest * 512, 512), 512)
        return remote(
            (q0, q1)[blk].at[:, to], qraw.at[blk, source], qs_sem.at[blk, n], qr_sem.at[blk, n], head=dest
        )

    for blk in range(2):
        for n, (dx, dc) in enumerate(Q_HOPS):
            copy = q_copy(blk, n, head_at(me, dx, dc), me)
            copy.start()
            sends.append(copy)
    for j in (1, NZ - 1):
        pl.semaphore_signal(near, inc=1, device_id={"ctx": ctx_at(y, z + j)}, device_id_type=MESH)

    kept_copy.wait()
    flags = jnp.where(
        (kept_ref[...] == lax.broadcasted_iota(jnp.int32, (32, 32), 0))
        & (lax.broadcasted_iota(jnp.int32, (32, 32), 1) < count_ref[0]),
        1.0, 0.0,
    )
    kept = jnp.max(flags, axis=1, keepdims=True)
    bias[0] = jnp.zeros((32, QT), F32)
    bias[1] = jnp.broadcast_to((1.0 - kept) * NEG, (32, QT))
    lz[...] = jnp.zeros(lz.shape, F32)

    kcopy.wait()
    prep_keys(kraw, kx, stage)
    vcopy.wait()
    prep_values(vraw, vt, stage)

    pl.semaphore_wait(near, 2)
    for j in (2, NZ - 2):
        pl.semaphore_signal(far, inc=1, device_id={"ctx": ctx_at(y, z + j)}, device_id_type=MESH)

    def arrived(blk, hops):
        for n, (dx, dc) in enumerate(Q_HOPS):
            if dx in hops:
                q_copy(blk, n, me, head_at(me, NX - dx, dc)).wait_recv()

    swap = (3 - (x + NX - y) % NX) // 3

    def spot(blk, chip):
        r = (chip + NX - (x, y)[blk]) % NX
        b1, b0 = r // 2, r % 2
        if blk == 0:
            return 2 * b1 + (b0 + b1) % 2
        high = 1 - (b0 + b1) % 2
        return 2 * high + (1 - b1 + swap * (1 - high)) % 2

    def prepare(blk, chip):
        for c in range(2):
            prep_queries(qraw, qx, blk, chip * 2 + c, spot(blk, chip) * 2 + c)

    def y_copy(blk, h, k, at):
        dest = ctx_at(y + k, z)
        at = pl.ds(pl.multiple_of(at * GRP, GRP), GRP)
        return (
            remote(obuf.at[blk, h, at, :], r1.at[blk, k - 1, h],
                   ys_sem.at[blk, h, k - 1], yr_sem.at[blk, h, k - 1], ctx=dest),
            remote(lse.at[blk, h, :, at], l1.at[blk, k - 1, h],
                   yls_sem.at[blk, h, k - 1], ylr_sem.at[blk, h, k - 1], ctx=dest),
        )

    def y_send(blk, h, p):
        if blk == 0:
            k = (x + (0, 1, 3, 2)[p] + NY - y) % NY

            @pl.when(k > 0)
            def _():
                for copy in y_copy(0, h, k, p):
                    copy.start()
        else:
            for copy in y_copy(1, h, (2 - swap, 1 + swap, 3)[p], p):
                copy.start()

    def y_arrive(blk, h):
        for k in range(1, NY):
            for copy in y_copy(blk, h, k, 0):
                copy.wait_recv()

    def z_copy(blk, h, j):
        to = (z + j) % NZ
        at = pl.ds(pl.multiple_of(to * OWN, 16), OWN)
        dest = ctx_at(y, to)
        return (
            remote(c1.at[blk, h, at, :], r2.at[blk, j - 1, h],
                   zs_sem.at[blk, h, j - 1], zr_sem.at[blk, h, j - 1], ctx=dest),
            remote(lz.at[blk, to, h], l2.at[blk, j - 1, h],
                   zls_sem.at[blk, h, j - 1], zlr_sem.at[blk, h, j - 1], ctx=dest),
        )

    def merge_y(blk, h):
        mine = pl.ds(pl.multiple_of(spot(blk, y) * GRP, GRP), GRP)
        y_arrive(blk, h)
        combine_y(blk, h, mine, obuf, lse, r1, l1, c1, lz)
        for j in (4, 3, 5, 2, 6, 1, 7):
            for copy in z_copy(blk, h, j):
                copy.start()

    def merge_z(blk, h):
        for j in range(1, NZ):
            for copy in z_copy(blk, h, j):
                copy.wait_recv()
        combine_z(blk, h, z, c1, lz, r2, l2, out)

    tile = make_tiles(kx, vt, qx, bias, obuf, lse, s0, s1)
    own[0].wait()
    arrived(0, (0,))
    prepare(0, x)
    m = tile(score=(0, 0))
    m = tile(score=(0, 1), value=(0, 0), m=m)

    due = {
        1: ((0, 0, 0),),
        2: ((0, 1, 0), (0, 0, 1)),
        3: ((0, 1, 1),),
        4: ((0, 0, 2),),
        5: ((0, 1, 2), (0, 0, 3)),
        6: ((0, 1, 3),),
        7: ((1, 0, 0),),
        8: ((1, 1, 0), (1, 0, 1)),
        9: ((1, 1, 1),),
    }

    def between(at):
        for blk, h, p in due.get(at, ()):
            y_send(blk, h, p)
        if at == 0:
            own[1].wait()
            arrived(1, (0,))
            prepare(1, x)
            arrived(0, (1, 3))
            prepare(0, (x + 1) % NX)
            prepare(0, (x + 3) % NX)
        if at == 3:
            arrived(0, (2,))
            prepare(0, (x + 2) % NX)
        if at == 5:
            arrived(1, (1, 3))
            prepare(1, (x + 1) % NX)
            prepare(1, (x + 3) % NX)
        if at == 6:
            arrived(1, (2,))
            prepare(1, (x + 2) % NX)

    def step(i, m):
        for at in range(10):

            @pl.when(i == at)
            def _():
                between(at)

        m = tile(score=(i + 1, 0), value=(i, 1), m=m)
        return tile(score=(i + 1, 1), value=(i + 1, 0), m=m)

    last = 2 * TILES - 1
    m = lax.fori_loop(0, last - 1, step, m)
    y_send(1, 0, 2)
    m = tile(score=(last, 0), value=(last - 1, 1), m=m)
    y_send(1, 1, 2)
    pl.semaphore_wait(far, 2)
    merge_y(0, 0)
    merge_y(0, 1)
    m = tile(score=(last, 1), value=(last, 0), m=m)
    tile(value=(last, 1), m=m)
    merge_y(1, 0)
    merge_y(1, 1)
    for blk in range(2):
        for h in range(KV):
            merge_z(blk, h)
    for copy in sends:
        copy.wait_send()
    for blk in range(2):
        for h in range(KV):
            for k in range(1, NY):
                for copy in y_copy(blk, h, k, 0):
                    copy.wait_send()
            for j in range(1, NZ):
                for copy in z_copy(blk, h, j):
                    copy.wait_send()


def shards(q_first, q_second, k_cache, v_cache, kept_blocks, kept_count):
    anyspace = pl.BlockSpec(memory_space=pl.ANY)
    vmem = pl.BlockSpec(memory_space=pltpu.VMEM)
    dma = pltpu.SemaphoreType.DMA
    both = pl.pallas_call(
        kernel,
        out_shape=jax.ShapeDtypeStruct((2, 24, 512), BF16),
        in_specs=[anyspace] * 5 + [pl.BlockSpec(memory_space=pltpu.SMEM)],
        out_specs=vmem,
        scratch_shapes=[
            pltpu.VMEM((KEYS * KV, HD), BF16),
            pltpu.VMEM((KEYS * KV, HD), BF16),
            pltpu.VMEM((2, 8, 96, 512), BF16),
            pltpu.VMEM((KV, KEYS, 2 * HD), BF16),
            pltpu.VMEM((KV, VROWS, KEYS), BF16),
            pltpu.VMEM((1024, HD), F32),
            pltpu.VMEM((2, KV, ROWS, 2 * HD), BF16),
            pltpu.VMEM((2, 32, QT), F32),
            pltpu.VMEM((KEYS, QT), F32),
            pltpu.VMEM((KEYS, QT), F32),
            pltpu.VMEM((2, KV, ROWS, HD), BF16),
            pltpu.VMEM((2, KV, 1, ROWS), F32),
            pltpu.VMEM((2, NY - 1, KV, GRP, HD), BF16),
            pltpu.VMEM((2, NY - 1, KV, 1, GRP), F32),
            pltpu.VMEM((2, KV, GRP, HD), BF16),
            pltpu.VMEM((2, NZ, KV, 1, 128), F32),
            pltpu.VMEM((2, NZ - 1, KV, OWN, HD), BF16),
            pltpu.VMEM((2, NZ - 1, KV, 1, 128), F32),
            dma((5,)),
            dma((2, 7)), dma((2, 7)),
            dma((2, KV, 3)), dma((2, KV, 3)), dma((2, KV, 3)), dma((2, KV, 3)),
            dma((2, KV, 7)), dma((2, KV, 7)), dma((2, KV, 7)), dma((2, KV, 7)),
            pltpu.SemaphoreType.REGULAR, pltpu.SemaphoreType.REGULAR,
            pltpu.VMEM((1, 32), jnp.int32),
        ],
        compiler_params=pltpu.CompilerParams(
            collective_id=0, has_side_effects=True, vmem_limit_bytes=60 * 1024 * 1024
        ),
    )(
        q_first, q_second,
        k_cache.reshape(KEYS * KV, HD), v_cache.reshape(KEYS * KV, HD),
        kept_blocks, kept_count,
    )
    return both[0], both[1]


def solution(mesh):
    placed = (
        P("head", None),
        P("head", None),
        P("ctx", "head", None),
        P("ctx", "head", None),
        P("ctx", None),
        P("ctx"),
    )
    return jax.shard_map(
        shards,
        mesh=mesh,
        in_specs=placed,
        out_specs=(P("ctx", "head"), P("ctx", "head")),
        check_vma=False,
    )
```

```python
import functools

import jax
import jax.numpy as jnp
from jax import lax
from jax.experimental import pallas as pl
from jax.experimental.pallas import tpu as pltpu
from jax.sharding import PartitionSpec as P

HD = 128
BLK = 128
F32 = jnp.float32
BF16 = jnp.bfloat16
SCALE = 168 ** -0.5 * 1.4426950408889634
NEG = -1e30
MESH = pl.DeviceIdType.MESH

KV = 2
KEYS = 4096
ROWS = 1536
QT = 256
TILES = ROWS // QT
CK = 1024
NB = KEYS // CK
NX, NY, NZ = 4, 4, 8
GRP = ROWS // NY
OWN = GRP // NZ
VROWS = HD + 16

Q_HOPS = ((0, 1), (1, 0), (1, 1), (3, 0), (3, 1), (2, 0), (2, 1))


def head_at(me, dx, dc):
    x, c = me // 2, me % 2
    return ((x + dx) % NX) * 2 + (c + dc) % 2


def ctx_at(y, z):
    return (y % NY) * NZ + z % NZ


def remote(src, dst, send_sem, recv_sem, **where):
    return pltpu.make_async_remote_copy(
        src_ref=src, dst_ref=dst, send_sem=send_sem, recv_sem=recv_sem, device_id=where, device_id_type=MESH
    )


def prep_keys(kraw, kx, stage):
    n = stage.shape[0]

    def step(i, c):
        stage[...] = kraw[pl.ds(i * n, n), :].astype(F32)
        for h in range(KV):
            k = stage[pl.ds(h, n // 2, stride=2), :].astype(BF16)
            rows = pl.ds(i * (n // 2), n // 2)
            kx[h, rows, 0:HD] = k
            kx[h, rows, HD : 2 * HD] = k
        return c

    lax.fori_loop(0, KEYS * KV // n, step, 0)


def prep_values(vraw, vt, stage):
    n = stage.shape[0]

    def step(i, c):
        stage[...] = vraw[pl.ds(i * n, n), :].astype(F32)
        for h in range(KV):
            v = stage[pl.ds(h, n // 2, stride=2), :].astype(BF16)
            vt[h, 0:HD, pl.ds(pl.multiple_of(i * (n // 2), n // 2), n // 2)] = v.T
        return c

    lax.fori_loop(0, KEYS * KV // n, step, 0)
    for h in range(KV):
        vt[h, HD:VROWS, :] = jnp.ones((VROWS - HD, KEYS), BF16)


def prep_queries(qraw, qx, blk, hs, pos):
    x = qraw[blk, hs].astype(F32) * SCALE
    rows = pl.ds(pl.multiple_of(pos * (4 * OWN), 64), 4 * OWN)
    for h in range(KV):
        a = x[:, h * 256 : h * 256 + 128]
        b = x[:, h * 256 + 128 : h * 256 + 256]
        pieces = []
        for j in range(4):
            pieces += [a[j * 24 : j * 24 + 24], b[j * 24 : j * 24 + 24]]
        full = jnp.concatenate(pieces, axis=0)
        hi = full.astype(BF16)
        qx[blk, h, rows, 0:HD] = hi
        qx[blk, h, rows, HD : 2 * HD] = (full - hi.astype(F32)).astype(BF16)


def scores_step(i, q, kx, h, s_ref, bias, blk, top):
    s = lax.dot_general(
        kx[h, pl.ds(i * CK, CK), :], q, (((1,), (1,)), ((), ())), preferred_element_type=F32
    )
    s_ref[pl.ds(i * CK, CK), :] = s
    for b in range(CK // BLK):
        part = s[b * BLK : (b + 1) * BLK].reshape(BLK // 8, 8, QT)
        top = jnp.maximum(top, jnp.max(part, axis=0) + bias[blk, pl.ds(i * (CK // BLK) + b, 1), :])
    return top


def values_step(i, vt, h, s_ref, bias, blk, top, total):
    pieces = []
    for b in range(CK // BLK):
        shift = top - bias[blk, pl.ds(i * (CK // BLK) + b, 1), :]
        pieces.append(jnp.exp2(s_ref[pl.ds(i * CK + b * BLK, BLK), :] - shift).astype(BF16))
    p = jnp.concatenate(pieces, axis=0)
    d = lax.dot_general(
        vt[h, :, pl.ds(i * CK, CK)], p, (((1,), (0,)), ((), ())), preferred_element_type=F32
    )
    return d if total is None else total + d


def make_tiles(kx, vt, qx, bias, obuf, lse, s0, s1):
    slots = (s0, s1)

    def cols(i):
        return pl.ds(pl.multiple_of((i % TILES) * QT, QT), QT)

    def finish(i, h, total, m):
        norm = total[HD : HD + 1, :]
        obuf[i // TILES, h, cols(i), :] = (total[0:HD, :] * (1.0 / norm)).T.astype(BF16)
        lse[i // TILES, h, :, cols(i)] = m + jnp.log2(norm)

    def run(score=None, value=None, m=None):
        top = jnp.full((8, QT), NEG, F32)
        total = None
        if score is not None:
            ia, ha = score
            q = qx[ia // TILES, ha, cols(ia), :]
        for n in range(NB):
            if score is not None:
                top = scores_step(n, q, kx, ha, slots[ha], bias, ia // TILES, top)
            if value is not None:
                ib, hb = value
                total = values_step(n, vt, hb, slots[hb], bias, ib // TILES, m, total)
        if value is not None:
            finish(ib, hb, total, m)
        return jnp.max(top, axis=0, keepdims=True)

    return run


def combine_y(blk, h, mine, obuf, lse, r1, l1, c1, lz):
    ls = [lse[blk, h, :, mine]] + [l1[blk, k, h] for k in range(NY - 1)]
    m = functools.reduce(jnp.maximum, ls)
    ws = [jnp.exp2(l - m) for l in ls]
    total = functools.reduce(jnp.add, ws)
    both = m + jnp.log2(total)
    for z in range(NZ):
        lz[blk, z, h, :, 0:OWN] = both[:, z * OWN : (z + 1) * OWN]
    w = jnp.concatenate([w / total for w in ws] * 2, axis=0).T
    acc = obuf[blk, h, mine, :].astype(F32) * w[:, 0:1]
    for k in range(NY - 1):
        acc += r1[blk, k, h].astype(F32) * w[:, k + 1 : k + 2]
    c1[blk, h] = acc.astype(BF16)


def combine_z(blk, h, z, c1, lz, r2, l2, out_ref):
    mine = pl.ds(pl.multiple_of(z * OWN, 16), OWN)
    ls = [lz[blk, z, h]] + [l2[blk, j, h] for j in range(NZ - 1)]
    m = functools.reduce(jnp.maximum, ls)
    ws = [jnp.exp2(l - m) for l in ls]
    total = functools.reduce(jnp.add, ws)
    w = jnp.concatenate([x / total for x in ws], axis=0).T
    acc = c1[blk, h, mine, :].astype(F32) * w[0:OWN, 0:1]
    for j in range(NZ - 1):
        acc += r2[blk, j, h].astype(F32) * w[0:OWN, j + 1 : j + 2]
    for g in range(2):
        at = (h * 2 + g) * HD
        out_ref[blk, :, at : at + HD] = acc[g * 24 : (g + 1) * 24].astype(BF16)


def kernel(
    q0, q1, k_hbm, v_hbm, kept_hbm, count_ref, out,
    kraw, vraw, qraw, kx, vt, stage, qx, bias, s0, s1, obuf, lse, r1, l1, c1, lz, r2, l2,
    local, qs_sem, qr_sem, ys_sem, yr_sem, yls_sem, ylr_sem, zs_sem, zr_sem, zls_sem, zlr_sem, near, far, kept_ref,
):
    me, ctx = lax.axis_index("head"), lax.axis_index("ctx")
    x, y, z = me // 2, ctx // NZ, ctx % NZ

    barrier = pltpu.get_barrier_semaphore()
    for dx, dc in Q_HOPS:
        pl.semaphore_signal(barrier, inc=1, device_id={"head": head_at(me, dx, dc)}, device_id_type=MESH)
    for k in range(1, NY):
        pl.semaphore_signal(barrier, inc=1, device_id={"ctx": ctx_at(y + k, z)}, device_id_type=MESH)
    for j in (1, NZ - 1):
        pl.semaphore_signal(barrier, inc=1, device_id={"ctx": ctx_at(y, z + j)}, device_id_type=MESH)

    kcopy = pltpu.make_async_copy(k_hbm, kraw, local.at[0])
    vcopy = pltpu.make_async_copy(v_hbm, vraw, local.at[1])
    own = []
    cols = pl.ds(pl.multiple_of(me * 512, 512), 512)
    for blk, q in enumerate((q0, q1)):
        own.append(pltpu.make_async_copy(q.at[:, cols], qraw.at[blk, me], local.at[2 + blk]))
    kept_copy = pltpu.make_async_copy(kept_hbm, kept_ref, local.at[4])
    own[0].start()
    kept_copy.start()
    kcopy.start()
    vcopy.start()
    own[1].start()

    pl.semaphore_wait(barrier, len(Q_HOPS) + NY - 1 + 2)

    sends = []

    def q_copy(blk, n, dest, source):
        to = pl.ds(pl.multiple_of(dest * 512, 512), 512)
        return remote(
            (q0, q1)[blk].at[:, to], qraw.at[blk, source], qs_sem.at[blk, n], qr_sem.at[blk, n], head=dest
        )

    for blk in range(2):
        for n, (dx, dc) in enumerate(Q_HOPS):
            copy = q_copy(blk, n, head_at(me, dx, dc), me)
            copy.start()
            sends.append(copy)
    for j in (1, NZ - 1):
        pl.semaphore_signal(near, inc=1, device_id={"ctx": ctx_at(y, z + j)}, device_id_type=MESH)

    kept_copy.wait()
    flags = jnp.where(
        (kept_ref[...] == lax.broadcasted_iota(jnp.int32, (32, 32), 0))
        & (lax.broadcasted_iota(jnp.int32, (32, 32), 1) < count_ref[0]),
        1.0, 0.0,
    )
    kept = jnp.max(flags, axis=1, keepdims=True)
    bias[0] = jnp.zeros((32, QT), F32)
    bias[1] = jnp.broadcast_to((1.0 - kept) * NEG, (32, QT))
    lz[...] = jnp.zeros(lz.shape, F32)

    kcopy.wait()
    prep_keys(kraw, kx, stage)
    vcopy.wait()
    prep_values(vraw, vt, stage)

    pl.semaphore_wait(near, 2)
    for j in (2, NZ - 2):
        pl.semaphore_signal(far, inc=1, device_id={"ctx": ctx_at(y, z + j)}, device_id_type=MESH)

    def arrived(blk, hops):
        for n, (dx, dc) in enumerate(Q_HOPS):
            if dx in hops:
                q_copy(blk, n, me, head_at(me, NX - dx, dc)).wait_recv()

    swap = (3 - (x + NX - y) % NX) // 3

    def spot(blk, chip):
        r = (chip + NX - (x, y)[blk]) % NX
        b1, b0 = r // 2, r % 2
        if blk == 0:
            return 2 * b1 + (b0 + b1) % 2
        high = 1 - (b0 + b1) % 2
        return 2 * high + (1 - b1 + swap * (1 - high)) % 2

    def prepare(blk, chip):
        for c in range(2):
            prep_queries(qraw, qx, blk, chip * 2 + c, spot(blk, chip) * 2 + c)

    def y_copy(blk, h, k, at):
        dest = ctx_at(y + k, z)
        at = pl.ds(pl.multiple_of(at * GRP, GRP), GRP)
        return (
            remote(obuf.at[blk, h, at, :], r1.at[blk, k - 1, h],
                   ys_sem.at[blk, h, k - 1], yr_sem.at[blk, h, k - 1], ctx=dest),
            remote(lse.at[blk, h, :, at], l1.at[blk, k - 1, h],
                   yls_sem.at[blk, h, k - 1], ylr_sem.at[blk, h, k - 1], ctx=dest),
        )

    def y_send(blk, h, p):
        if blk == 0:
            k = (x + (0, 1, 3, 2)[p] + NY - y) % NY

            @pl.when(k > 0)
            def _():
                for copy in y_copy(0, h, k, p):
                    copy.start()
        else:
            for copy in y_copy(1, h, (2 - swap, 1 + swap)[p], p):
                copy.start()

    def y_tail(h, part):
        off, n = ((0, QT), (QT, GRP - QT))[part]
        dest = ctx_at(y + 3, z)
        made = [remote(obuf.at[1, h, pl.ds(2 * GRP + off, n), :], r1.at[1, 2, h, pl.ds(off, n), :],
                       ys_sem.at[1, h, 2 + part], yr_sem.at[1, h, 2 + part], ctx=dest)]
        if part:
            made.append(remote(lse.at[1, h, :, pl.ds(2 * GRP, GRP)], l1.at[1, 2, h],
                               yls_sem.at[1, h, 2], ylr_sem.at[1, h, 2], ctx=dest))
        return made

    def y_tail_send(h, part):
        for copy in y_tail(h, part):
            copy.start()

    def y_all(blk, h):
        copies = []
        for k in range(1, NY):
            if blk == 1 and k == 3:
                copies += y_tail(h, 0) + y_tail(h, 1)
            else:
                copies += y_copy(blk, h, k, 0)
        return copies

    def y_arrive(blk, h):
        for copy in y_all(blk, h):
            copy.wait_recv()

    def z_copy(blk, h, j):
        to = (z + j) % NZ
        at = pl.ds(pl.multiple_of(to * OWN, 16), OWN)
        dest = ctx_at(y, to)
        return (
            remote(c1.at[blk, h, at, :], r2.at[blk, j - 1, h],
                   zs_sem.at[blk, h, j - 1], zr_sem.at[blk, h, j - 1], ctx=dest),
            remote(lz.at[blk, to, h], l2.at[blk, j - 1, h],
                   zls_sem.at[blk, h, j - 1], zlr_sem.at[blk, h, j - 1], ctx=dest),
        )

    def merge_y(blk, h):
        mine = pl.ds(pl.multiple_of(spot(blk, y) * GRP, GRP), GRP)
        y_arrive(blk, h)
        combine_y(blk, h, mine, obuf, lse, r1, l1, c1, lz)
        for j in (4, 3, 5, 2, 6, 1, 7):
            for copy in z_copy(blk, h, j):
                copy.start()

    def merge_z(blk, h):
        for j in range(1, NZ):
            for copy in z_copy(blk, h, j):
                copy.wait_recv()
        combine_z(blk, h, z, c1, lz, r2, l2, out)

    tile = make_tiles(kx, vt, qx, bias, obuf, lse, s0, s1)
    own[0].wait()
    arrived(0, (0,))
    prepare(0, x)
    m = tile(score=(0, 0))
    m = tile(score=(0, 1), value=(0, 0), m=m)

    due = {
        1: ((0, 0, 0),),
        2: ((0, 1, 0), (0, 0, 1)),
        3: ((0, 1, 1),),
        4: ((0, 0, 2),),
        5: ((0, 1, 2), (0, 0, 3)),
        6: ((0, 1, 3),),
        7: ((1, 0, 0),),
        8: ((1, 1, 0), (1, 0, 1)),
        9: ((1, 1, 1),),
    }

    def between(at):
        for blk, h, p in due.get(at, ()):
            y_send(blk, h, p)
        if at == 0:
            own[1].wait()
            arrived(1, (0,))
            prepare(1, x)
            arrived(0, (1, 3))
            prepare(0, (x + 1) % NX)
            prepare(0, (x + 3) % NX)
        if at == 3:
            arrived(0, (2,))
            prepare(0, (x + 2) % NX)
        if at == 5:
            arrived(1, (1, 3))
            prepare(1, (x + 1) % NX)
            prepare(1, (x + 3) % NX)
        if at == 6:
            arrived(1, (2,))
            prepare(1, (x + 2) % NX)
        if at == 9:
            y_tail_send(0, 0)

    def step(i, m):
        for at in range(10):

            @pl.when(i == at)
            def _():
                between(at)

        m = tile(score=(i + 1, 0), value=(i, 1), m=m)
        return tile(score=(i + 1, 1), value=(i + 1, 0), m=m)

    last = 2 * TILES - 1
    m = lax.fori_loop(0, last - 1, step, m)
    y_tail_send(0, 1)
    y_tail_send(1, 0)
    m = tile(score=(last, 0), value=(last - 1, 1), m=m)
    y_tail_send(1, 1)
    pl.semaphore_wait(far, 2)
    merge_y(0, 0)
    merge_y(0, 1)
    m = tile(score=(last, 1), value=(last, 0), m=m)
    tile(value=(last, 1), m=m)
    merge_y(1, 0)
    merge_y(1, 1)
    for blk in range(2):
        for h in range(KV):
            merge_z(blk, h)
    for copy in sends:
        copy.wait_send()
    for blk in range(2):
        for h in range(KV):
            for copy in y_all(blk, h):
                copy.wait_send()
            for j in range(1, NZ):
                for copy in z_copy(blk, h, j):
                    copy.wait_send()


def shards(q_first, q_second, k_cache, v_cache, kept_blocks, kept_count):
    anyspace = pl.BlockSpec(memory_space=pl.ANY)
    vmem = pl.BlockSpec(memory_space=pltpu.VMEM)
    dma = pltpu.SemaphoreType.DMA
    both = pl.pallas_call(
        kernel,
        out_shape=jax.ShapeDtypeStruct((2, 24, 512), BF16),
        in_specs=[anyspace] * 5 + [pl.BlockSpec(memory_space=pltpu.SMEM)],
        out_specs=vmem,
        scratch_shapes=[
            pltpu.VMEM((KEYS * KV, HD), BF16),
            pltpu.VMEM((KEYS * KV, HD), BF16),
            pltpu.VMEM((2, 8, 96, 512), BF16),
            pltpu.VMEM((KV, KEYS, 2 * HD), BF16),
            pltpu.VMEM((KV, VROWS, KEYS), BF16),
            pltpu.VMEM((1024, HD), F32),
            pltpu.VMEM((2, KV, ROWS, 2 * HD), BF16),
            pltpu.VMEM((2, 32, QT), F32),
            pltpu.VMEM((KEYS, QT), F32),
            pltpu.VMEM((KEYS, QT), F32),
            pltpu.VMEM((2, KV, ROWS, HD), BF16),
            pltpu.VMEM((2, KV, 1, ROWS), F32),
            pltpu.VMEM((2, NY - 1, KV, GRP, HD), BF16),
            pltpu.VMEM((2, NY - 1, KV, 1, GRP), F32),
            pltpu.VMEM((2, KV, GRP, HD), BF16),
            pltpu.VMEM((2, NZ, KV, 1, 128), F32),
            pltpu.VMEM((2, NZ - 1, KV, OWN, HD), BF16),
            pltpu.VMEM((2, NZ - 1, KV, 1, 128), F32),
            dma((5,)),
            dma((2, 7)), dma((2, 7)),
            dma((2, KV, 4)), dma((2, KV, 4)), dma((2, KV, 3)), dma((2, KV, 3)),
            dma((2, KV, 7)), dma((2, KV, 7)), dma((2, KV, 7)), dma((2, KV, 7)),
            pltpu.SemaphoreType.REGULAR, pltpu.SemaphoreType.REGULAR,
            pltpu.VMEM((1, 32), jnp.int32),
        ],
        compiler_params=pltpu.CompilerParams(
            collective_id=0, has_side_effects=True, vmem_limit_bytes=60 * 1024 * 1024
        ),
    )(
        q_first, q_second,
        k_cache.reshape(KEYS * KV, HD), v_cache.reshape(KEYS * KV, HD),
        kept_blocks, kept_count,
    )
    return both[0], both[1]


def solution(mesh):
    placed = (
        P("head", None),
        P("head", None),
        P("ctx", "head", None),
        P("ctx", "head", None),
        P("ctx", None),
        P("ctx"),
    )
    return jax.shard_map(
        shards,
        mesh=mesh,
        in_specs=placed,
        out_specs=(P("ctx", "head"), P("ctx", "head")),
        check_vma=False,
    )
```
